128 devices in a mesh: node: 8 (over z, core), chip: 16 (over y, x).
Axes of the slice: x: 4, y: 4, z: 4, core: 2. Of those that a mesh axis runs over, the one named last changes fastest.
Arguments:
- tokens: bfloat16 [2048, 3584], P(('node', 'chip')), may hold values from -6 to 6
- expert_ids: int32 [2048, 8], P(('node', 'chip')), may hold values from 0 to 127, all different within a row; in each aligned block of 16 rows (0 to 15, 16 to 31, ...) at most 2 rows name the same one
- route_weight: float32 [2048, 8], P(('node', 'chip')), may hold values from 0.1 to 1
- expert_gate: bfloat16 [128, 3584, 1024], P(('node', 'chip')), may hold values from -0.09375 to 0.09375
- expert_up: bfloat16 [128, 3584, 1024], P(('node', 'chip')), may hold values from -0.09375 to 0.09375
- expert_down: bfloat16 [128, 1024, 3584], P(('node', 'chip')), may hold values from -0.1875 to 0.1875
- shared_gate: bfloat16 [3584, 2048], P(None, 'chip'), may hold values from -0.09375 to 0.09375
- shared_up: bfloat16 [3584, 2048], P(None, 'chip'), may hold values from -0.09375 to 0.09375
- shared_down: bfloat16 [2048, 3584], P('chip'), may hold values from -0.125 to 0.125
- query_latent: bfloat16 [512, 64, 512], P(('node', 'chip')), may hold values from -32 to 32
- query_rope: bfloat16 [512, 4096], P(('node', 'chip')), may hold values from -4 to 4
- cache_latent: bfloat16 [512, 128, 512], P(('node', 'chip')), may hold values from -8 to 8
- cache_rope: bfloat16 [512, 64, 128], P(('node', 'chip')), may hold values from -4 to 4
- cache_len: int32 [512], P(('node', 'chip')), may hold values from 2 to 128
Outputs:
- moe_out: bfloat16 [2048, 3584], P(('node', 'chip'))
- attn_out: bfloat16 [512, 64, 512], P(('node', 'chip'))
The draws below stay inside these ranges and needn't reach their ends.
Inputs may be any that keep to these rules, and one draw needn't show every extreme that they name: `expert_ids`: a row names 8 different experts; the rows of one device name any one expert at most 2 times, a bound that some block reaches.
All inputs are finite; a program needn't handle non-finite values.
Results may differ from the reference program's by a relative error of at most 0.0085.
Values may be sent and summed in bfloat16 or wider, within the bound.
No kernel may reach another device: no remote copies, remote signals or barrier semaphores. Data moves between devices by JAX's collectives and lax.ppermute only.
A program may use at most 128 MiB of HBM per device.

```python
import math
import jax
import jax.numpy as jnp
import numpy as np
from jax import lax

D = 3584
FF = 1024
FFS = 2048
TOPK = 8
HEADS = 64
LATENT = 512
ROPE = 64
TOK_DEV = 16
CACHE = 128
EXPERTS = 128
CAP = 2
TOKENS = 2048
ALL_SEQS = 512
N_NODE = 8
N_CHIP = 16


def latent_fields(key):
    key_list = jax.random.split(jax.random.fold_in(key, 7), 3)
    cache_vals = jnp.clip(jax.random.normal(key_list[0], (ALL_SEQS, CACHE, LATENT), jnp.float32), -4.0, 4.0)
    queries = jnp.clip(jax.random.normal(key_list[1], (ALL_SEQS, HEADS, LATENT), jnp.float32), -4.0, 4.0)
    rope_vals = jnp.clip(jax.random.normal(key_list[2], (ALL_SEQS, HEADS * ROPE), jnp.float32), -4.0, 4.0)
    return (queries, rope_vals, cache_vals)


def draw_query_latent(key, part):
    return latent_fields(key)[0].astype(jnp.bfloat16)


def draw_query_rope(key, part):
    return latent_fields(key)[1].astype(jnp.bfloat16)


def draw_cache_latent(key, part):
    return latent_fields(key)[2].astype(jnp.bfloat16)


def touch_ends(entries, stream_key, least, high):
    shape = entries.shape
    index_at = [jax.random.randint(jax.random.fold_in(stream_key, axis), (), 0, shape[axis]) for axis in range(len(shape))]
    entries = entries.at[tuple(index_at)].set(least)
    longest = shape.index(max(shape))
    index_at[longest] = (index_at[longest] + 1) % shape[longest]
    return entries.at[tuple(index_at)].set(high)


def shard_levels(own_key, shape, cuts, least, high):
    gain, own = 1.0, jax.random.fold_in(own_key, 6)
    for dim, parts in cuts:
        heights = jnp.exp(jax.random.uniform(jax.random.fold_in(own, dim), (parts,), jnp.float32, least / len(cuts), high / len(cuts)))
        gain = gain * jnp.repeat(heights, shape[dim] // parts).reshape([-1 if axis == dim else 1 for axis in range(len(shape))])
    return gain


def deal_out(stream_key, own, number, rows, count, top, limit, skew):
    ranking = jax.random.permutation(stream_key, count)
    packed, common = shares(count, rows * top, limit, skew, True), shares(count, rows * top, limit, skew, False)
    places = jnp.arange(count)

    def named(lengths, turn):
        used = int((lengths > 0).sum())
        fixed = max(1, used // 4)
        passed = fixed + (places - fixed + turn * (used - fixed)) % max(1, count - fixed)
        return jnp.zeros((count,), jnp.int32).at[ranking[jnp.where(places < fixed, places, passed)]].set(jnp.asarray(lengths, jnp.int32))

    lengths = jnp.where(number % 4 == 0, named(packed, number // 4), named(common, number - number // 4 - 1))
    mixed = jax.random.permutation(jax.random.fold_in(own, 3), count)
    source_of, sink = mixed[0:count // 2 * 2:2], mixed[1:count // 2 * 2:2]
    room = jnp.minimum(lengths[source_of] - 1, limit - lengths[sink]) // 2
    room = jnp.where((source_of == ranking[0]) | (sink == ranking[0]) | (lengths[sink] == 0), 0, jnp.maximum(room, 0))
    passed = jax.random.randint(jax.random.fold_in(own, 4), (count // 2,), 0, 1 << 20) % (room + 1)
    lengths = lengths.at[source_of].add(-passed).at[sink].add(passed)
    members = jnp.searchsorted(jnp.cumsum(lengths), jnp.arange(rows * top), side="right").astype(jnp.int32)
    grid = members.reshape(top, rows).T
    grid = grid[jax.random.permutation(jax.random.fold_in(own, 1), rows)]
    turn = jax.random.randint(jax.random.fold_in(own, 2), (rows, 1), 0, top)
    return jnp.take_along_axis(grid, (jnp.arange(top)[None, :] + turn) % top, axis=1)


def shares(count, total, bound, slope, full):
    portions = [(1 << 20) // math.isqrt(grade ** slope) + 1 for grade in range(1, count + 1)]
    largest = bound if full else min(bound, max(-(-total // count), total * portions[0] // sum(portions)))
    least = 1 if total - largest >= count - 1 else 0
    given, spare = [largest] + [least] * (count - 1), total - largest - least * (count - 1)
    while spare > 0:
        free = [i for i in range(1, count) if given[i] < largest] or [i for i in range(1, count) if given[i] < bound]
        whole, budget = sum([portions[i] for i in free]), spare
        for i in free:
            extra = min(bound - given[i], max(1, budget * portions[i] // whole), spare)
            given[i] = given[i] + extra
            spare = spare - extra
    return np.array(given)


def noise(stream_key, extent, scale, limit, shards=(), kind=jnp.bfloat16):
    level = shard_levels(stream_key, extent, shards, -0.22, 0.18) if shards else 1.0
    entries = jax.random.normal(stream_key, extent, jnp.float32) * scale * level
    return jnp.minimum(jnp.maximum(entries, -limit), limit).astype(kind)


def setup_inputs(seed: int = 0) -> dict:
    keys = jax.random.split(jax.random.key(seed), 15)
    tokens = noise(keys[0], (TOKENS, D), 1.0, 6.0, ((0, 128),))
    expert_ids_keys = jax.random.split(jax.random.fold_in(keys[1], 1), TOKENS // TOK_DEV)
    expert_ids_turns = jax.random.permutation(jax.random.fold_in(keys[1], 3), TOKENS // TOK_DEV)
    expert_ids = jax.vmap(lambda own, number: deal_out(jax.random.fold_in(keys[1], 2), own, number, TOK_DEV, EXPERTS, TOPK, CAP, 2))(expert_ids_keys, expert_ids_turns).reshape((TOKENS, TOPK))
    route_weight = jnp.clip(jnp.exp(math.log(1.0) - 2.3025851 * jax.random.uniform(keys[2], (TOKENS, TOPK), jnp.float32) ** shard_levels(keys[2], (TOKENS, TOPK), ((0, 128),), -0.2, 0.2)), 0.1, 1.0)
    expert_gate = noise(keys[3], (EXPERTS, D, FF), D ** -0.5, 0.09375, ((0, 128),))
    expert_up = noise(keys[4], (EXPERTS, D, FF), D ** -0.5, 0.09375, ((0, 128),))
    expert_down = noise(keys[5], (EXPERTS, FF, D), FF ** -0.5, 0.1875, ((0, 128),))
    shared_gate = noise(keys[6], (D, FFS), D ** -0.5, 0.09375, ((1, 16),))
    shared_up = noise(keys[7], (D, FFS), D ** -0.5, 0.09375, ((1, 16),))
    shared_down = noise(keys[8], (FFS, D), FFS ** -0.5, 0.125, ((0, 16),))
    query_latent = draw_query_latent(jax.random.fold_in(keys[14], 71), 0)
    query_rope = draw_query_rope(jax.random.fold_in(keys[14], 71), 0)
    cache_latent = draw_cache_latent(jax.random.fold_in(keys[14], 71), 0)
    cache_rope = noise(keys[12], (ALL_SEQS, ROPE, CACHE), 1.0, 4.0, ((0, 128),))
    cache_len = touch_ends(jax.random.randint(keys[13], (ALL_SEQS,), 2, CACHE + 1), jax.random.fold_in(keys[13], 1), 2, CACHE).astype(jnp.int32)
    return dict(tokens=tokens, expert_ids=expert_ids, route_weight=route_weight, expert_gate=expert_gate, expert_up=expert_up, expert_down=expert_down, shared_gate=shared_gate, shared_up=shared_up, shared_down=shared_down, query_latent=query_latent, query_rope=query_rope, cache_latent=cache_latent, cache_rope=cache_rope, cache_len=cache_len)


score_scale = 192.0 ** -0.5


def swiglu_hidden(token_rows, gate_matrix, up_matrix):
    gate_part = jnp.dot(token_rows, gate_matrix, preferred_element_type=jnp.float32)
    up_part = jnp.dot(token_rows, up_matrix, preferred_element_type=jnp.float32)
    return (jax.nn.silu(gate_part) * up_part).astype(jnp.bfloat16)


def attend(query_latent, query_rope, cache_latent, cache_rope, cache_len):
    seq_count, head_count, latent_width = query_latent.shape
    rope_width = cache_rope.shape[1]
    cache_size = cache_rope.shape[2]
    rope_query = query_rope.reshape(seq_count, head_count, rope_width).astype(jnp.float32)
    cache_float = cache_latent.astype(jnp.float32)
    scores = jnp.einsum("shl,spl->shp", query_latent.astype(jnp.float32), cache_float)
    scores = scores + jnp.einsum("shr,srp->shp", rope_query, cache_rope.astype(jnp.float32))
    scores = scores * score_scale
    position = jnp.arange(cache_size, dtype=jnp.int32)
    live_mask = position[None, None, :] < cache_len[:, None, None]
    masked = jnp.where(live_mask, scores, -1e30)
    row_peak = jnp.max(masked, axis=2, keepdims=True)
    weight = jnp.where(live_mask, jnp.exp(masked - row_peak), 0.0)
    softmax_weight = (weight / jnp.sum(weight, axis=2, keepdims=True)).astype(jnp.bfloat16)
    attended = jnp.einsum("shp,spl->shl", softmax_weight.astype(jnp.float32), cache_float)
    return attended.astype(jnp.bfloat16)


def reference(tokens, expert_ids, route_weight, expert_gate, expert_up, expert_down, shared_gate, shared_up, shared_down, query_latent, query_rope, cache_latent, cache_rope, cache_len):
    experts = N_NODE * N_CHIP
    devices = experts
    model_width = tokens.shape[1]
    per_device = TOK_DEV * TOPK
    flat_ids = expert_ids.reshape(devices, per_device).astype(jnp.int32)
    onehot = (flat_ids[:, :, None] == jnp.arange(experts, dtype=jnp.int32)[None, None, :]).astype(jnp.int32)
    earlier = jnp.cumsum(onehot, axis=1) - onehot
    slot_index = jnp.sum(earlier * onehot, axis=2).astype(jnp.int32)
    source = jnp.broadcast_to(jnp.arange(devices, dtype=jnp.int32)[:, None], (devices, per_device))
    assign = jnp.arange(devices * per_device, dtype=jnp.int32).reshape(devices, per_device)
    slot_table = jnp.full((experts, devices, CAP), -1, jnp.int32).at[flat_ids, source, slot_index].set(assign)
    weights_flat = route_weight.reshape(-1)

    def one_expert(totals, expert_index):
        owner_slots = slot_table[expert_index].reshape(-1)
        live_slot = owner_slots >= 0
        safe_index = jnp.where(live_slot, owner_slots, 0).astype(jnp.int32)
        token_index = (safe_index // TOPK).astype(jnp.int32)
        hidden = swiglu_hidden(tokens[token_index], expert_gate[expert_index], expert_up[expert_index])
        result = jnp.dot(hidden, expert_down[expert_index], preferred_element_type=jnp.float32).astype(jnp.bfloat16)
        scale_row = jnp.where(live_slot, weights_flat[safe_index], jnp.zeros((), jnp.float32))
        totals = totals.at[token_index].add(scale_row[:, None] * result.astype(jnp.float32))
        return totals, None

    routed, _ = lax.scan(one_expert, jnp.zeros((tokens.shape[0], model_width), jnp.float32), jnp.arange(experts, dtype=jnp.int32))
    shared_hidden = swiglu_hidden(tokens, shared_gate, shared_up)
    shared_out = jnp.dot(shared_hidden, shared_down, preferred_element_type=jnp.float32)
    moe_out = (shared_out + routed).astype(jnp.bfloat16)
    attn_out = attend(query_latent, query_rope, cache_latent, cache_rope, cache_len)
    return (moe_out, attn_out)
```

```python
import jax
import jax.numpy as jnp
from jax import lax
from jax.experimental import pallas as pl
from jax.experimental.pallas import tpu as pltpu
from jax.sharding import PartitionSpec as P


TOPK = 8
SIDE = 4
META = 128
SLOTS = 32
MIB = 1 << 20

score_scale = 192.0 ** (-0.5)
bf16 = jnp.bfloat16
f32 = jnp.float32


def x_pairs(step):
    return [(y * SIDE + x, y * SIDE + (x + step) % SIDE) for y in range(SIDE) for x in range(SIDE)]


def y_pairs(step):
    return [(y * SIDE + x, (y + step) % SIDE * SIDE + x) for y in range(SIDE) for x in range(SIDE)]


def z_pairs(step, swap):
    return [(z * 2 + k, (z + step) % SIDE * 2 + (k ^ swap)) for z in range(SIDE) for k in range(2)]


TARGETS = [(step, swap) for step in range(SIDE) for swap in range(2)]


def kernel(body, outs, name, flops, moved, limit, scratch=(), **more):
    return pl.pallas_call(
        body,
        out_shape=[jax.ShapeDtypeStruct(shape, kind) for shape, kind in outs],
        scratch_shapes=list(scratch),
        name=name,
        cost_estimate=pl.CostEstimate(flops=flops, bytes_accessed=moved, transcendentals=0),
        compiler_params=pltpu.CompilerParams(vmem_limit_bytes=limit),
        **more,
    )


def pack_body(tokens_ref, meta_ref, a_ref, b_ref):
    half = b_ref.shape[1]
    a_ref[:, :half] = tokens_ref[:, :half]
    b_ref[...] = tokens_ref[:, half:]
    value = meta_ref[...]
    high = value.astype(bf16).astype(f32)
    low = value - high
    lane = lax.broadcasted_iota(jnp.int32, value.shape, 1)
    a_ref[:, half:] = jnp.where(lane < 2 * TOPK, high, low).astype(bf16)


def select_body(expert_ref, *refs):
    a_refs, b_refs = refs[:SIDE], refs[SIDE : 2 * SIDE]
    x_ref, high_ref, low_ref = refs[2 * SIDE : 2 * SIDE + 3]
    row_refs = refs[2 * SIDE + 3 :]
    half = b_refs[0].shape[1]
    group = a_refs[0].shape[0]
    rows = group // SIDE
    for dy in range(SIDE):
        x_ref[dy * group : (dy + 1) * group, :half] = a_refs[dy][:, :half]
        for dx in range(SIDE):
            at = (dy * SIDE + dx) * rows
            x_ref[at : at + rows, half:] = b_refs[dx][dy * rows : (dy + 1) * rows, :]
    meta = jnp.concatenate([ref[:, half:] for ref in a_refs], axis=0).astype(f32)
    count, lanes = meta.shape[0], high_ref.shape[1]
    wanted = expert_ref[...]
    named = jnp.zeros((count, lanes), f32)
    high = jnp.zeros((count, lanes), f32)
    low = jnp.zeros((count, lanes), f32)
    for k in range(TOPK):
        hit = meta[:, k : k + 1] == wanted
        named = named + jnp.where(hit, 1.0, 0.0)
        high = high + jnp.where(hit, meta[:, TOPK + k : TOPK + k + 1], 0.0)
        low = low + jnp.where(hit, meta[:, 2 * TOPK + k : 2 * TOPK + k + 1], 0.0)
    above = lax.broadcasted_iota(jnp.int32, (count, count), 1)
    below = lax.broadcasted_iota(jnp.int32, (count, count), 0)
    earlier = jnp.where(above < below, 1.0, 0.0).astype(bf16)
    place = jnp.dot(earlier, named.astype(bf16), preferred_element_type=f32)
    slot = (lax.broadcasted_iota(jnp.int32, (count, lanes), 1) % SLOTS).astype(f32)
    here = place == slot
    chosen = jnp.where(here, named, 0.0)
    high_ref[...] = jnp.where(here, high, 0.0).astype(bf16)
    low_ref[...] = jnp.where(here, low, 0.0).astype(bf16)
    pick = chosen.T.astype(bf16)
    width = x_ref.shape[1]
    tile = 512
    for c in range(0, width, tile):
        picked = jnp.dot(pick, x_ref[:, c : c + tile], preferred_element_type=f32).astype(bf16)
        for t, ref in enumerate(row_refs):
            ref[:, c : c + tile] = picked[t * SLOTS : (t + 1) * SLOTS]


def silu_times(gate_part, up_part):
    return (gate_part / (1.0 + jnp.exp(-gate_part)) * up_part).astype(bf16)


def shared_body(x_ref, gate_ref, up_ref, out_ref):
    rows = x_ref[...]
    gate_part = jnp.dot(rows, gate_ref[...], preferred_element_type=f32)
    up_part = jnp.dot(rows, up_ref[...], preferred_element_type=f32)
    out_ref[...] = silu_times(gate_part, up_part)


def expert_body(*refs):
    count = len(TARGETS)
    row_refs = refs[:count]
    gate_ref, up_ref, down_ref = refs[count : count + 3]
    out_refs = refs[count + 3 : 2 * count + 3]
    x_ref, total_ref = refs[2 * count + 3 :]
    step = pl.program_id(0)
    last = pl.num_programs(0) - 1

    @pl.when(step == 0)
    def _():
        for t, ref in enumerate(row_refs):
            x_ref[t * SLOTS : (t + 1) * SLOTS, :] = ref[...]

    rows = x_ref[...]
    gate_part = jnp.dot(rows, gate_ref[0], preferred_element_type=f32)
    up_part = jnp.dot(rows, up_ref[0], preferred_element_type=f32)
    hidden = silu_times(gate_part, up_part)
    width = x_ref.shape[1]
    tile = 512
    for c in range(0, width, tile):
        term = jnp.dot(hidden, down_ref[0, :, c : c + tile], preferred_element_type=f32)

        @pl.when(step == 0)
        def _():
            total_ref[:, c : c + tile] = term

        @pl.when(jnp.logical_and(step > 0, step < last))
        def _():
            total_ref[:, c : c + tile] = total_ref[:, c : c + tile] + term

        @pl.when(step == last)
        def _():
            total = (total_ref[:, c : c + tile] + term).astype(bf16)
            for t, ref in enumerate(out_refs):
                ref[:, c : c + tile] = total[t * SLOTS : (t + 1) * SLOTS]


def combine_body(high_ref, low_ref, hidden_ref, down_ref, *refs):
    count = len(TARGETS)
    back_refs = refs[:count]
    a_refs, b_refs = refs[count : count + SIDE], refs[count + SIDE : count + 2 * SIDE]
    half = b_refs[0].shape[1]
    group = a_refs[0].shape[0]
    rows = group // SIDE
    high, low, hidden = high_ref[...], low_ref[...], hidden_ref[...]
    tile = 256
    for c in range(0, 2 * half, tile):
        back = jnp.concatenate([ref[:, c : c + tile] for ref in back_refs], axis=0)
        total = jnp.dot(hidden, down_ref[:, c : c + tile], preferred_element_type=f32)
        total = total + jnp.dot(high, back, preferred_element_type=f32)
        total = (total + jnp.dot(low, back, preferred_element_type=f32)).astype(bf16)
        if c < half:
            for dy in range(SIDE):
                a_refs[dy][:, c : c + tile] = total[dy * group : (dy + 1) * group]
        else:
            for dx in range(SIDE):
                for dy in range(SIDE):
                    at = (dy * SIDE + dx) * rows
                    b_refs[dx][dy * rows : (dy + 1) * rows, c - half : c - half + tile] = total[at : at + rows]


def fold_body(*refs):
    in_refs, out_refs = refs[:SIDE], refs[SIDE:]
    rows = out_refs[0].shape[0]
    for j, ref in enumerate(out_refs):
        parts = [r[j * rows : (j + 1) * rows, :].astype(f32) for r in in_refs]
        ref[...] = sum(parts[1:], parts[0]).astype(bf16)


def finish_body(*refs):
    a_refs, b_refs, out_ref = refs[:SIDE], refs[SIDE : 2 * SIDE], refs[2 * SIDE]
    half = b_refs[0].shape[1]
    a = [r[...].astype(f32) for r in a_refs]
    b = [r[...].astype(f32) for r in b_refs]
    out_ref[:, :half] = sum(a[1:], a[0]).astype(bf16)
    out_ref[:, half:] = sum(b[1:], b[0]).astype(bf16)


def attend(query_latent, query_rope, cache_latent, cache_rope, cache_len):
    seq_count, head_count, latent_width = query_latent.shape
    rope_width = cache_rope.shape[1]
    cache_size = cache_rope.shape[2]
    rope_query = query_rope.reshape(seq_count, head_count, rope_width)
    scores = jnp.einsum(
        "shl,spl->shp", query_latent, cache_latent, preferred_element_type=jnp.float32
    )
    scores = scores + jnp.einsum(
        "shr,srp->shp", rope_query, cache_rope, preferred_element_type=jnp.float32
    )
    scores = scores * score_scale
    position = jnp.arange(cache_size, dtype=jnp.int32)
    live_mask = position[None, None, :] < cache_len[:, None, None]
    masked = jnp.where(live_mask, scores, -1e30)
    row_peak = jnp.max(masked, axis=2, keepdims=True)
    weight = jnp.where(live_mask, jnp.exp(masked - row_peak), 0.0)
    softmax_weight = (weight / jnp.sum(weight, axis=2, keepdims=True)).astype(jnp.bfloat16)
    attended = jnp.einsum(
        "shp,spl->shl", softmax_weight, cache_latent, preferred_element_type=jnp.float32
    )
    return attended.astype(jnp.bfloat16)


def local(
    tokens,
    expert_ids,
    route_weight,
    expert_gate,
    expert_up,
    expert_down,
    shared_gate,
    shared_up,
    shared_down,
    query_latent,
    query_rope,
    cache_latent,
    cache_rope,
    cache_len,
):
    rows, width = tokens.shape
    half = width // 2
    group = SIDE * rows
    whole = SIDE * group
    ff = expert_gate.shape[2]
    hidden_width = shared_gate.shape[1]
    weight_bytes = 2 * width * ff

    def along(value, pairs):
        return lax.ppermute(value, "chip", pairs)

    meta = jnp.concatenate([expert_ids.astype(f32), route_weight, route_weight], axis=1)
    meta = jnp.pad(meta, ((0, 0), (0, META - 3 * TOPK)))
    own_a, own_b = kernel(
        pack_body, [((rows, half + META), bf16), ((rows, half), bf16)], "pack", 10**5, 4 * rows * width, 4 * MIB
    )(tokens, meta)
    row_a = jnp.concatenate([own_a] + [along(own_a, x_pairs(-d)) for d in range(1, SIDE)], axis=0)
    row_b = jnp.concatenate([own_b] + [along(own_b, y_pairs(-d)) for d in range(1, SIDE)], axis=0)
    all_a = [row_a] + [along(row_a, y_pairs(-d)) for d in range(1, SIDE)]
    all_b = [row_b] + [along(row_b, x_pairs(-d)) for d in range(1, SIDE)]

    node, chip = lax.axis_index("node"), lax.axis_index("chip")
    lane = jnp.arange(len(TARGETS) * SLOTS, dtype=jnp.int32)
    target = lane // SLOTS
    to_node = (node // 2 + target // 2) % SIDE * 2 + (node % 2 + target % 2) % 2
    wanted = (to_node * (SIDE * SIDE) + chip).astype(f32)[None, :]
    slots = len(TARGETS) * SLOTS
    picked = kernel(
        select_body,
        [((whole, width), bf16), ((whole, slots), bf16), ((whole, slots), bf16)]
        + [((SLOTS, width), bf16)] * len(TARGETS),
        "select",
        2 * whole * slots * width,
        8 * whole * width,
        24 * MIB,
    )(wanted, *all_a, *all_b)
    plane_tokens, high, low = picked[:3]
    arrived = [
        lax.ppermute(block, "node", z_pairs(*t)) if t != (0, 0) else block
        for t, block in zip(TARGETS, picked[3:])
    ]

    (hidden,) = kernel(
        shared_body,
        [((whole, hidden_width), bf16)],
        "shared",
        4 * whole * width * hidden_width,
        4 * width * hidden_width,
        24 * MIB,
    )(plane_tokens, shared_gate, shared_up)

    block_ff = 256
    full = pl.BlockSpec((SLOTS, width), lambda j: (0, 0))
    answers = pl.pallas_call(
        expert_body,
        grid=(ff // block_ff,),
        in_specs=[full] * len(TARGETS)
        + [
            pl.BlockSpec((1, width, block_ff), lambda j: (0, 0, j)),
            pl.BlockSpec((1, width, block_ff), lambda j: (0, 0, j)),
            pl.BlockSpec((1, block_ff, width), lambda j: (0, j, 0)),
        ],
        out_specs=[full] * len(TARGETS),
        out_shape=[jax.ShapeDtypeStruct((SLOTS, width), bf16)] * len(TARGETS),
        scratch_shapes=[pltpu.VMEM((slots, width), bf16), pltpu.VMEM((slots, width), f32)],
        name="expert",
        cost_estimate=pl.CostEstimate(
            flops=6 * slots * width * ff, bytes_accessed=3 * weight_bytes, transcendentals=slots * ff
        ),
        compiler_params=pltpu.CompilerParams(
            vmem_limit_bytes=40 * MIB, dimension_semantics=("arbitrary",)
        ),
    )(*arrived, expert_gate, expert_up, expert_down)
    returned = [
        lax.ppermute(block, "node", z_pairs(-t[0], t[1])) if t != (0, 0) else block
        for t, block in zip(TARGETS, answers)
    ]

    partial = kernel(
        combine_body,
        [((group, half), bf16)] * (2 * SIDE),
        "combine",
        2 * whole * (2 * slots + hidden_width) * width,
        8 * whole * width,
        24 * MIB,
    )(high, low, hidden, shared_down, *returned)
    part_a, part_b = partial[:SIDE], partial[SIDE:]
    from_y = [part_a[0]] + [along(part_a[d], y_pairs(d)) for d in range(1, SIDE)]
    from_x = [part_b[0]] + [along(part_b[d], x_pairs(d)) for d in range(1, SIDE)]
    fold = kernel(fold_body, [((rows, half), bf16)] * SIDE, "fold", 10**6, 4 * group * width, 8 * MIB)
    fold_a, fold_b = fold(*from_y), fold(*from_x)
    last_a = [fold_a[0]] + [along(fold_a[d], x_pairs(d)) for d in range(1, SIDE)]
    last_b = [fold_b[0]] + [along(fold_b[d], y_pairs(d)) for d in range(1, SIDE)]
    (moe_out,) = kernel(
        finish_body, [((rows, width), bf16)], "finish", 10**6, 10 * rows * width, 4 * MIB
    )(*last_a, *last_b)
    attn_out = attend(query_latent, query_rope, cache_latent, cache_rope, cache_len)
    return (moe_out, attn_out)


def solution(mesh):
    placed = (
        P(("node", "chip"), None),
        P(("node", "chip"), None),
        P(("node", "chip"), None),
        P(("node", "chip"), None, None),
        P(("node", "chip"), None, None),
        P(("node", "chip"), None, None),
        P(None, "chip"),
        P(None, "chip"),
        P("chip", None),
        P(("node", "chip"), None, None),
        P(("node", "chip"), None),
        P(("node", "chip"), None, None),
        P(("node", "chip"), None, None),
        P(("node", "chip")),
    )
    return jax.shard_map(
        local,
        mesh=mesh,
        in_specs=placed,
        out_specs=(P(("node", "chip"), None), P(("node", "chip"), None, None)),
        check_vma=False,
    )
```

```python
import jax
import jax.numpy as jnp
from jax import lax
from jax.experimental import pallas as pl
from jax.experimental.pallas import tpu as pltpu
from jax.sharding import PartitionSpec as P


TOPK = 8
SIDE = 4
META = 128
SLOTS = 32
MIB = 1 << 20

score_scale = 192.0 ** (-0.5)
bf16 = jnp.bfloat16
f32 = jnp.float32


def plane_pairs(first, step):
    pairs = []
    for z in range(SIDE):
        for k in range(2):
            for y in range(SIDE):
                for x in range(SIDE):
                    along_x = first == (k == 0)
                    to = (y, (x + step) % SIDE) if along_x else ((y + step) % SIDE, x)
                    node = (z * 2 + k) * SIDE * SIDE
                    pairs.append((node + y * SIDE + x, node + to[0] * SIDE + to[1]))
    return pairs


def z_pairs(step, swap):
    return [(z * 2 + k, (z + step) % SIDE * 2 + (k ^ swap)) for z in range(SIDE) for k in range(2)]


TARGETS = [(step, swap) for step in range(SIDE) for swap in range(2)]


def kernel(body, outs, flops, moved, limit, scratch=(), **more):
    return pl.pallas_call(
        body,
        out_shape=[jax.ShapeDtypeStruct(shape, kind) for shape, kind in outs],
        scratch_shapes=list(scratch),
        cost_estimate=pl.CostEstimate(flops=flops, bytes_accessed=moved, transcendentals=0),
        compiler_params=pltpu.CompilerParams(vmem_limit_bytes=limit),
        **more,
    )


def pack_body(tokens_ref, meta_ref, out_ref):
    width = tokens_ref.shape[1]
    out_ref[:, :width] = tokens_ref[...]
    value = meta_ref[...]
    high = value.astype(bf16).astype(f32)
    low = value - high
    lane = lax.broadcasted_iota(jnp.int32, value.shape, 1)
    out_ref[:, width:] = jnp.where(lane < 2 * TOPK, high, low).astype(bf16)


def select_body(expert_ref, *refs):
    block_refs = refs[:SIDE]
    x_ref, high_ref, low_ref = refs[SIDE : SIDE + 3]
    row_refs = refs[SIDE + 3 :]
    width = x_ref.shape[1]
    group = block_refs[0].shape[0]
    for j, ref in enumerate(block_refs):
        x_ref[j * group : (j + 1) * group, :] = ref[:, :width]
    meta = jnp.concatenate([ref[:, width:] for ref in block_refs], axis=0).astype(f32)
    count, lanes = meta.shape[0], high_ref.shape[1]
    wanted = expert_ref[...]
    named = jnp.zeros((count, lanes), f32)
    high = jnp.zeros((count, lanes), f32)
    low = jnp.zeros((count, lanes), f32)
    for k in range(TOPK):
        hit = meta[:, k : k + 1] == wanted
        named = named + jnp.where(hit, 1.0, 0.0)
        high = high + jnp.where(hit, meta[:, TOPK + k : TOPK + k + 1], 0.0)
        low = low + jnp.where(hit, meta[:, 2 * TOPK + k : 2 * TOPK + k + 1], 0.0)
    above = lax.broadcasted_iota(jnp.int32, (count, count), 1)
    below = lax.broadcasted_iota(jnp.int32, (count, count), 0)
    earlier = jnp.where(above < below, 1.0, 0.0).astype(bf16)
    place = jnp.dot(earlier, named.astype(bf16), preferred_element_type=f32)
    slot = (lax.broadcasted_iota(jnp.int32, (count, lanes), 1) % SLOTS).astype(f32)
    here = place == slot
    chosen = jnp.where(here, named, 0.0)
    high_ref[...] = jnp.where(here, high, 0.0).astype(bf16)
    low_ref[...] = jnp.where(here, low, 0.0).astype(bf16)
    pick = chosen.T.astype(bf16)
    tile = 512
    for c in range(0, width, tile):
        picked = jnp.dot(pick, x_ref[:, c : c + tile], preferred_element_type=f32).astype(bf16)
        for t, ref in enumerate(row_refs):
            ref[:, c : c + tile] = picked[t * SLOTS : (t + 1) * SLOTS]


def load_body(gate_ref, up_ref, down_ref, rows_ref, gate_out, up_out, down_out, sems):
    copies = [
        pltpu.make_async_copy(gate_ref.at[0], gate_out, sems.at[0]),
        pltpu.make_async_copy(up_ref.at[0], up_out, sems.at[1]),
        pltpu.make_async_copy(down_ref.at[0], down_out, sems.at[2]),
    ]
    for copy in copies:
        copy.start()
    for copy in copies:
        copy.wait()


def silu_times(gate_part, up_part):
    return (gate_part / (1.0 + jnp.exp(-gate_part)) * up_part).astype(bf16)


def shared_body(x_ref, gate_ref, up_ref, out_ref):
    rows = x_ref[...]
    gate_part = jnp.dot(rows, gate_ref[...], preferred_element_type=f32)
    up_part = jnp.dot(rows, up_ref[...], preferred_element_type=f32)
    out_ref[...] = silu_times(gate_part, up_part)


def expert_body(*refs):
    count = len(TARGETS)
    row_refs = refs[:count]
    gate_ref, up_ref, down_ref = refs[count : count + 3]
    out_refs = refs[count + 3 : 2 * count + 3]
    x_ref, hidden_ref = refs[2 * count + 3 :]
    for t, ref in enumerate(row_refs):
        x_ref[t * SLOTS : (t + 1) * SLOTS, :] = ref[...]
    width, ff = gate_ref.shape
    tile = 256
    for c in range(0, ff, tile):
        rows = x_ref[...]
        gate_part = jnp.dot(rows, gate_ref[:, c : c + tile], preferred_element_type=f32)
        up_part = jnp.dot(rows, up_ref[:, c : c + tile], preferred_element_type=f32)
        hidden_ref[:, c : c + tile] = silu_times(gate_part, up_part)
    for c in range(0, width, tile):
        hidden = hidden_ref[...]
        result = jnp.dot(hidden, down_ref[:, c : c + tile], preferred_element_type=f32).astype(bf16)
        for t, ref in enumerate(out_refs):
            ref[:, c : c + tile] = result[t * SLOTS : (t + 1) * SLOTS]


def combine_body(attended_ref, high_ref, low_ref, hidden_ref, down_ref, *refs):
    count = len(TARGETS)
    back_refs, out_refs = refs[:count], refs[count:]
    group, width = out_refs[0].shape
    high, low, hidden = high_ref[...], low_ref[...], hidden_ref[...]
    tile = 256
    for c in range(0, width, tile):
        back = jnp.concatenate([ref[:, c : c + tile] for ref in back_refs], axis=0)
        total = jnp.dot(hidden, down_ref[:, c : c + tile], preferred_element_type=f32)
        total = total + jnp.dot(high, back, preferred_element_type=f32)
        total = (total + jnp.dot(low, back, preferred_element_type=f32)).astype(bf16)
        for j, ref in enumerate(out_refs):
            ref[:, c : c + tile] = total[j * group : (j + 1) * group]


def fold_body(*refs):
    in_refs, out_refs = refs[:SIDE], refs[SIDE:]
    rows = out_refs[0].shape[0]
    for j, ref in enumerate(out_refs):
        parts = [r[j * rows : (j + 1) * rows, :].astype(f32) for r in in_refs]
        ref[...] = sum(parts[1:], parts[0]).astype(bf16)


def attend_body(len_ref, query_ref, rope_query_ref, cache_ref, rope_ref, answer_ref, out_ref):
    seqs, heads, _ = query_ref.shape
    rope, _ = rope_ref.shape[1:]
    pair = 2 * rope
    for s in range(seqs):
        head = lax.broadcasted_iota(jnp.int32, (heads, pair), 0)
        high = lax.broadcasted_iota(jnp.int32, (heads, pair), 1) // rope
        rows = jnp.zeros((heads, pair), f32)
        for j in range(heads // 2):
            line = rope_query_ref[s : s + 1, j * pair : (j + 1) * pair].astype(f32)
            rows = jnp.where(head == 2 * j + high, line, rows)
        twice = jnp.concatenate([rope_ref[s], rope_ref[s]], axis=0)
        cache = cache_ref[s]
        scores = lax.dot_general(
            query_ref[s], cache, (((1,), (1,)), ((), ())), preferred_element_type=f32
        )
        scores = scores + jnp.dot(rows.astype(bf16), twice, preferred_element_type=f32)
        scores = scores * score_scale
        live = lax.broadcasted_iota(jnp.int32, scores.shape, 1) < len_ref[s]
        masked = jnp.where(live, scores, -1e30)
        peak = jnp.max(masked, axis=1, keepdims=True)
        weight = jnp.where(live, jnp.exp(masked - peak), 0.0)
        weight = (weight / jnp.sum(weight, axis=1, keepdims=True)).astype(bf16)
        out_ref[s] = jnp.dot(weight, cache, preferred_element_type=f32).astype(bf16)


def local(
    tokens,
    expert_ids,
    route_weight,
    expert_gate,
    expert_up,
    expert_down,
    shared_gate,
    shared_up,
    shared_down,
    query_latent,
    query_rope,
    cache_latent,
    cache_rope,
    cache_len,
):
    rows, width = tokens.shape
    group = SIDE * rows
    whole = SIDE * group
    ff = expert_gate.shape[2]
    hidden_width = shared_gate.shape[1]
    weight_bytes = 2 * width * ff

    def along(value, first, step):
        return lax.ppermute(value, ("node", "chip"), plane_pairs(first, step))

    meta = jnp.concatenate([expert_ids.astype(f32), route_weight, route_weight], axis=1)
    meta = jnp.pad(meta, ((0, 0), (0, META - 3 * TOPK)))
    (own,) = kernel(
        pack_body, [((rows, width + META), bf16)], 10**5, 4 * rows * width, 4 * MIB
    )(tokens, meta)
    line = jnp.concatenate([own] + [along(own, True, -d) for d in range(1, SIDE)], axis=0)
    plane = [line] + [along(line, False, -d) for d in range(1, SIDE)]

    node, chip = lax.axis_index("node"), lax.axis_index("chip")
    lane = jnp.arange(len(TARGETS) * SLOTS, dtype=jnp.int32)
    target = lane // SLOTS
    to_node = (node // 2 + target // 2) % SIDE * 2 + (node % 2 + target % 2) % 2
    wanted = (to_node * (SIDE * SIDE) + chip).astype(f32)[None, :]
    slots = len(TARGETS) * SLOTS
    picked = kernel(
        select_body,
        [((whole, width), bf16), ((whole, slots), bf16), ((whole, slots), bf16)]
        + [((SLOTS, width), bf16)] * len(TARGETS),
        2 * whole * slots * width,
        8 * whole * width,
        12 * MIB,
    )(wanted, *plane)
    plane_tokens, high, low = picked[:3]
    arrived = [
        lax.ppermute(block, "node", z_pairs(*t)) if t != (0, 0) else block
        for t, block in zip(TARGETS, picked[3:])
    ]

    (hidden,) = kernel(
        shared_body,
        [((whole, hidden_width), bf16)],
        4 * whole * width * hidden_width,
        4 * width * hidden_width,
        8 * MIB,
    )(plane_tokens, shared_gate, shared_up)

    in_vmem = pl.BlockSpec(memory_space=pltpu.VMEM)
    anywhere = pl.BlockSpec(memory_space=pl.ANY)
    loaded = pl.pallas_call(
        load_body,
        in_specs=[anywhere] * 4,
        out_specs=[in_vmem] * 3,
        out_shape=[
            pltpu.VMEM((width, ff), bf16),
            pltpu.VMEM((width, ff), bf16),
            pltpu.VMEM((ff, width), bf16),
        ],
        scratch_shapes=[pltpu.SemaphoreType.DMA((3,))],
        name="load",
        cost_estimate=pl.CostEstimate(
            flops=6 * slots * width * ff, bytes_accessed=6 * weight_bytes, transcendentals=0
        ),
        compiler_params=pltpu.CompilerParams(vmem_limit_bytes=34 * MIB),
    )(expert_gate, expert_up, expert_down, picked[3])
    answers = kernel(
        expert_body,
        [((SLOTS, width), bf16)] * len(TARGETS),
        6 * slots * width * ff,
        3 * weight_bytes,
        12 * MIB,
        scratch=(pltpu.VMEM((slots, width), bf16), pltpu.VMEM((slots, ff), bf16)),
        in_specs=[in_vmem] * (len(TARGETS) + 3),
    )(*arrived, *loaded)
    returned = [
        lax.ppermute(block, "node", z_pairs(-t[0], t[1])) if t != (0, 0) else block
        for t, block in zip(TARGETS, answers)
    ]

    (attn_out,) = kernel(
        attend_body,
        [(query_latent.shape, bf16)],
        4 * query_latent.size * cache_rope.shape[2],
        4 * query_latent.size + 2 * cache_latent.size,
        6 * MIB,
        in_specs=[pl.BlockSpec(memory_space=pltpu.SMEM)] + [in_vmem] * 4 + [anywhere],
    )(cache_len, query_latent, query_rope, cache_latent, cache_rope, answers[0])

    partial = kernel(
        combine_body,
        [((group, width), bf16)] * SIDE,
        2 * whole * (2 * slots + hidden_width) * width,
        8 * whole * width,
        12 * MIB,
        in_specs=[anywhere] + [in_vmem] * (4 + len(TARGETS)),
    )(attn_out, high, low, hidden, shared_down, *returned)
    lines = [partial[0]] + [along(partial[d], False, d) for d in range(1, SIDE)]
    folded = kernel(fold_body, [((rows, width), bf16)] * SIDE, 10**6, 8 * group * width, 8 * MIB)(*lines)
    last = [folded[0]] + [along(folded[d], True, d) for d in range(1, SIDE)]
    (moe_out,) = kernel(
        fold_body, [((rows, width), bf16)], 10**6, 10 * rows * width, 4 * MIB
    )(*last)
    return (moe_out, attn_out)


def solution(mesh):
    placed = (
        P(("node", "chip"), None),
        P(("node", "chip"), None),
        P(("node", "chip"), None),
        P(("node", "chip"), None, None),
        P(("node", "chip"), None, None),
        P(("node", "chip"), None, None),
        P(None, "chip"),
        P(None, "chip"),
        P("chip", None),
        P(("node", "chip"), None, None),
        P(("node", "chip"), None),
        P(("node", "chip"), None, None),
        P(("node", "chip"), None, None),
        P(("node", "chip")),
    )

    return jax.shard_map(
        local,
        mesh=mesh,
        in_specs=placed,
        out_specs=(P(("node", "chip"), None), P(("node", "chip"), None, None)),
        check_vma=False,
    )
```

```python
import jax
import jax.numpy as jnp
from jax import lax
from jax.experimental import pallas as pl
from jax.experimental.pallas import tpu as pltpu
from jax.sharding import PartitionSpec as P


TOPK = 8
SIDE = 4
META = 128
SLOTS = 32
MIB = 1 << 20

score_scale = 192.0 ** (-0.5)
bf16 = jnp.bfloat16
f32 = jnp.float32
MARK = ((8, 128), f32)


def plane_pairs(first, step):
    pairs = []
    for z in range(SIDE):
        for k in range(2):
            for y in range(SIDE):
                for x in range(SIDE):
                    along_x = first == (k == 0)
                    to = (y, (x + step) % SIDE) if along_x else ((y + step) % SIDE, x)
                    node = (z * 2 + k) * SIDE * SIDE
                    pairs.append((node + y * SIDE + x, node + to[0] * SIDE + to[1]))
    return pairs


def z_pairs(step, swap):
    return [(z * 2 + k, (z + step) % SIDE * 2 + (k ^ swap)) for z in range(SIDE) for k in range(2)]


TARGETS = [(step, swap) for step in range(SIDE) for swap in range(2)]


def kernel(body, outs, flops, moved, limit, scratch=(), **more):
    return pl.pallas_call(
        body,
        out_shape=[out if isinstance(out, pl.MemoryRef) else jax.ShapeDtypeStruct(*out) for out in outs],
        scratch_shapes=list(scratch),
        cost_estimate=pl.CostEstimate(flops=flops, bytes_accessed=moved, transcendentals=0),
        compiler_params=pltpu.CompilerParams(vmem_limit_bytes=limit),
        **more,
    )


def pack_body(tokens_ref, ids_from, weight_from, out_ref, ids_ref, weight_ref, sems):
    rows, width = tokens_ref.shape
    copies = [
        pltpu.make_async_copy(ids_from, ids_ref, sems.at[0]),
        pltpu.make_async_copy(weight_from, weight_ref, sems.at[1]),
        pltpu.make_async_copy(tokens_ref, out_ref.at[:, :width], sems.at[2]),
    ]
    for copy in copies:
        copy.start()
    copies[0].wait()
    copies[1].wait()
    value = weight_ref[...]
    high = value.astype(bf16).astype(f32)
    parts = [ids_ref[...].astype(f32), high, value - high, jnp.zeros((TOPK, rows), f32)]
    meta = jnp.concatenate(parts, axis=0).astype(bf16)
    part = lax.broadcasted_iota(jnp.int32, (4 * TOPK, META), 0)
    lane = lax.broadcasted_iota(jnp.int32, (4 * TOPK, META), 1)
    spread = jnp.where(part == lane, 1.0, 0.0).astype(bf16)
    out_ref[:, width:] = lax.dot_general(
        meta, spread, (((0,), (0,)), ((), ())), preferred_element_type=f32
    ).astype(bf16)
    copies[2].wait()


def select_body(expert_ref, *refs):
    block_refs = refs[:SIDE]
    x_ref, high_ref, low_ref = refs[SIDE : SIDE + 3]
    row_refs, mark_ref = refs[SIDE + 3 : -1], refs[-1]
    mark_ref[...] = jnp.zeros(mark_ref.shape, f32)
    width = x_ref.shape[1]
    group = block_refs[0].shape[0]
    for j, ref in enumerate(block_refs):
        x_ref[j * group : (j + 1) * group, :] = ref[:, :width]
    meta = jnp.concatenate([ref[:, width:] for ref in block_refs], axis=0).astype(f32)
    count, lanes = meta.shape[0], high_ref.shape[1]
    wanted = expert_ref[...]
    named = jnp.zeros((count, lanes), f32)
    high = jnp.zeros((count, lanes), f32)
    low = jnp.zeros((count, lanes), f32)
    for k in range(TOPK):
        hit = meta[:, k : k + 1] == wanted
        named = named + jnp.where(hit, 1.0, 0.0)
        high = high + jnp.where(hit, meta[:, TOPK + k : TOPK + k + 1], 0.0)
        low = low + jnp.where(hit, meta[:, 2 * TOPK + k : 2 * TOPK + k + 1], 0.0)
    above = lax.broadcasted_iota(jnp.int32, (count, count), 1)
    below = lax.broadcasted_iota(jnp.int32, (count, count), 0)
    earlier = jnp.where(above < below, 1.0, 0.0).astype(bf16)
    place = jnp.dot(earlier, named.astype(bf16), preferred_element_type=f32)
    slot = (lax.broadcasted_iota(jnp.int32, (count, lanes), 1) % SLOTS).astype(f32)
    here = place == slot
    chosen = jnp.where(here, named, 0.0)
    high_ref[...] = jnp.where(here, high, 0.0).astype(bf16)
    low_ref[...] = jnp.where(here, low, 0.0).astype(bf16)
    pick = chosen.T.astype(bf16)
    tile = 512
    for c in range(0, width, tile):
        picked = jnp.dot(pick, x_ref[:, c : c + tile], preferred_element_type=f32).astype(bf16)
        for t, ref in enumerate(row_refs):
            ref[:, c : c + tile] = picked[t * SLOTS : (t + 1) * SLOTS]


def load_body(gate_ref, up_ref, down_ref, rows_ref, gate_out, up_out, down_out, sems):
    copies = [
        pltpu.make_async_copy(gate_ref.at[0], gate_out, sems.at[0]),
        pltpu.make_async_copy(up_ref.at[0], up_out, sems.at[1]),
        pltpu.make_async_copy(down_ref.at[0], down_out, sems.at[2]),
    ]
    for copy in copies:
        copy.start()
    for copy in copies:
        copy.wait()


def silu_times(gate_part, up_part):
    return (gate_part / (1.0 + jnp.exp(-gate_part)) * up_part).astype(bf16)


def shared_body(x_ref, gate_ref, up_ref, out_ref):
    rows = x_ref[...]
    gate_part = jnp.dot(rows, gate_ref[...], preferred_element_type=f32)
    up_part = jnp.dot(rows, up_ref[...], preferred_element_type=f32)
    out_ref[...] = silu_times(gate_part, up_part)


def expert_body(*refs):
    count = len(TARGETS)
    row_refs = refs[:count]
    gate_ref, up_ref, down_ref = refs[count : count + 3]
    out_refs = refs[count + 3 : 2 * count + 3]
    mark_ref, x_ref, hidden_ref = refs[2 * count + 3 :]
    mark_ref[...] = jnp.zeros(mark_ref.shape, f32)
    for t, ref in enumerate(row_refs):
        x_ref[t * SLOTS : (t + 1) * SLOTS, :] = ref[...]
    width, ff = gate_ref.shape
    tile = 256
    for c in range(0, ff, tile):
        rows = x_ref[...]
        gate_part = jnp.dot(rows, gate_ref[:, c : c + tile], preferred_element_type=f32)
        up_part = jnp.dot(rows, up_ref[:, c : c + tile], preferred_element_type=f32)
        hidden_ref[:, c : c + tile] = silu_times(gate_part, up_part)
    for c in range(0, width, tile):
        hidden = hidden_ref[...]
        result = jnp.dot(hidden, down_ref[:, c : c + tile], preferred_element_type=f32).astype(bf16)
        for t, ref in enumerate(out_refs):
            ref[:, c : c + tile] = result[t * SLOTS : (t + 1) * SLOTS]


def combine_body(attended_ref, high_ref, low_ref, hidden_ref, down_ref, *refs):
    count = len(TARGETS)
    back_refs, out_refs = refs[:count], refs[count:]
    group, width = out_refs[0].shape
    high, low, hidden = high_ref[...], low_ref[...], hidden_ref[...]
    tile = 256
    for c in range(0, width, tile):
        back = jnp.concatenate([ref[:, c : c + tile] for ref in back_refs], axis=0)
        total = jnp.dot(hidden, down_ref[:, c : c + tile], preferred_element_type=f32)
        total = total + jnp.dot(high, back, preferred_element_type=f32)
        total = (total + jnp.dot(low, back, preferred_element_type=f32)).astype(bf16)
        for j, ref in enumerate(out_refs):
            ref[:, c : c + tile] = total[j * group : (j + 1) * group]


def fold_body(*refs):
    in_refs, out_refs = refs[:SIDE], refs[SIDE:]
    rows = out_refs[0].shape[0]
    for j, ref in enumerate(out_refs):
        parts = [r[j * rows : (j + 1) * rows, :].astype(f32) for r in in_refs]
        ref[...] = sum(parts[1:], parts[0]).astype(bf16)


def attend_body(len_ref, query_ref, rope_query_ref, cache_ref, rope_ref, answer_ref, out_ref, mark_ref):
    mark_ref[...] = jnp.zeros(mark_ref.shape, f32)
    seqs, heads, _ = query_ref.shape
    rope, _ = rope_ref.shape[1:]
    pair = 2 * rope
    for s in range(seqs):
        head = lax.broadcasted_iota(jnp.int32, (heads, pair), 0)
        high = lax.broadcasted_iota(jnp.int32, (heads, pair), 1) // rope
        rows = jnp.zeros((heads, pair), f32)
        for j in range(heads // 2):
            line = rope_query_ref[s : s + 1, j * pair : (j + 1) * pair].astype(f32)
            rows = jnp.where(head == 2 * j + high, line, rows)
        twice = jnp.concatenate([rope_ref[s], rope_ref[s]], axis=0)
        cache = cache_ref[s]
        scores = lax.dot_general(
            query_ref[s], cache, (((1,), (1,)), ((), ())), preferred_element_type=f32
        )
        scores = scores + jnp.dot(rows.astype(bf16), twice, preferred_element_type=f32)
        scores = scores * score_scale
        live = lax.broadcasted_iota(jnp.int32, scores.shape, 1) < len_ref[s]
        masked = jnp.where(live, scores, -1e30)
        peak = jnp.max(masked, axis=1, keepdims=True)
        weight = jnp.where(live, jnp.exp(masked - peak), 0.0)
        weight = (weight / jnp.sum(weight, axis=1, keepdims=True)).astype(bf16)
        out_ref[s] = jnp.dot(weight, cache, preferred_element_type=f32).astype(bf16)


def local(
    tokens,
    expert_ids,
    route_weight,
    expert_gate,
    expert_up,
    expert_down,
    shared_gate,
    shared_up,
    shared_down,
    query_latent,
    query_rope,
    cache_latent,
    cache_rope,
    cache_len,
):
    rows, width = tokens.shape
    group = SIDE * rows
    whole = SIDE * group
    ff = expert_gate.shape[2]
    hidden_width = shared_gate.shape[1]
    weight_bytes = 2 * width * ff

    def along(value, first, step):
        return lax.ppermute(value, ("node", "chip"), plane_pairs(first, step))

    anywhere = pl.BlockSpec(memory_space=pl.ANY)
    in_vmem = pl.BlockSpec(memory_space=pltpu.VMEM)
    (own,) = kernel(
        pack_body,
        [pltpu.VMEM((rows, width + META), bf16)],
        10**5,
        4 * rows * width,
        56 * MIB,
        scratch=(
            pltpu.VMEM((TOPK, rows), jnp.int32),
            pltpu.VMEM((TOPK, rows), f32),
            pltpu.SemaphoreType.DMA((3,)),
        ),
        in_specs=[anywhere] * 3,
        out_specs=[in_vmem],
    )(tokens, expert_ids.T, route_weight.T)
    line = jnp.concatenate([own] + [along(own, True, -d) for d in range(1, SIDE)], axis=0)
    plane = [line] + [along(line, False, -d) for d in range(1, SIDE)]

    node, chip = lax.axis_index("node"), lax.axis_index("chip")
    lane = jnp.arange(len(TARGETS) * SLOTS, dtype=jnp.int32)
    target = lane // SLOTS
    to_node = (node // 2 + target // 2) % SIDE * 2 + (node % 2 + target % 2) % 2
    wanted = (to_node * (SIDE * SIDE) + chip).astype(f32)[None, :]
    slots = len(TARGETS) * SLOTS
    picked = kernel(
        select_body,
        [((whole, width), bf16), ((whole, slots), bf16), ((whole, slots), bf16)]
        + [((SLOTS, width), bf16)] * len(TARGETS)
        + [MARK],
        2 * whole * slots * width,
        8 * whole * width,
        12 * MIB,
    )(wanted, *plane)
    plane_tokens, high, low = picked[:3]
    arrived = [
        lax.ppermute(block, "node", z_pairs(*t)) if t != (0, 0) else block
        for t, block in zip(TARGETS, picked[3:-1])
    ]

    (hidden,) = kernel(
        shared_body,
        [((whole, hidden_width), bf16)],
        4 * whole * width * hidden_width,
        4 * width * hidden_width,
        8 * MIB,
    )(plane_tokens, shared_gate, shared_up)

    loaded = pl.pallas_call(
        load_body,
        in_specs=[anywhere] * 3 + [in_vmem],
        out_specs=[in_vmem] * 3,
        out_shape=[
            pltpu.VMEM((width, ff), bf16),
            pltpu.VMEM((width, ff), bf16),
            pltpu.VMEM((ff, width), bf16),
        ],
        scratch_shapes=[pltpu.SemaphoreType.DMA((3,))],
        name="load",
        cost_estimate=pl.CostEstimate(
            flops=6 * slots * width * ff, bytes_accessed=6 * weight_bytes, transcendentals=0
        ),
        compiler_params=pltpu.CompilerParams(vmem_limit_bytes=34 * MIB),
    )(expert_gate, expert_up, expert_down, picked[-1])
    *answers, answered = kernel(
        expert_body,
        [((SLOTS, width), bf16)] * len(TARGETS) + [MARK],
        6 * slots * width * ff,
        3 * weight_bytes,
        12 * MIB,
        scratch=(pltpu.VMEM((slots, width), bf16), pltpu.VMEM((slots, ff), bf16)),
        in_specs=[in_vmem] * (len(TARGETS) + 3),
    )(*arrived, *loaded)
    returned = [
        lax.ppermute(block, "node", z_pairs(-t[0], t[1])) if t != (0, 0) else block
        for t, block in zip(TARGETS, answers)
    ]

    attn_out, attended = kernel(
        attend_body,
        [(query_latent.shape, bf16), MARK],
        4 * query_latent.size * cache_rope.shape[2],
        4 * query_latent.size + 2 * cache_latent.size,
        6 * MIB,
        in_specs=[pl.BlockSpec(memory_space=pltpu.SMEM)] + [in_vmem] * 5,
    )(cache_len, query_latent, query_rope, cache_latent, cache_rope, answered)

    partial = kernel(
        combine_body,
        [((group, width), bf16)] * SIDE,
        2 * whole * (2 * slots + hidden_width) * width,
        8 * whole * width,
        12 * MIB,
        in_specs=[in_vmem] * (5 + len(TARGETS)),
    )(attended, high, low, hidden, shared_down, *returned)
    lines = [partial[0]] + [along(partial[d], False, d) for d in range(1, SIDE)]
    folded = kernel(fold_body, [((rows, width), bf16)] * SIDE, 10**6, 8 * group * width, 8 * MIB)(*lines)
    last = [folded[0]] + [along(folded[d], True, d) for d in range(1, SIDE)]
    (moe_out,) = kernel(
        fold_body, [((rows, width), bf16)], 10**6, 10 * rows * width, 4 * MIB
    )(*last)
    return (moe_out, attn_out)


def solution(mesh):
    placed = (
        P(("node", "chip"), None),
        P(("node", "chip"), None),
        P(("node", "chip"), None),
        P(("node", "chip"), None, None),
        P(("node", "chip"), None, None),
        P(("node", "chip"), None, None),
        P(None, "chip"),
        P(None, "chip"),
        P("chip", None),
        P(("node", "chip"), None, None),
        P(("node", "chip"), None),
        P(("node", "chip"), None, None),
        P(("node", "chip"), None, None),
        P(("node", "chip")),
    )

    return jax.shard_map(
        local,
        mesh=mesh,
        in_specs=placed,
        out_specs=(P(("node", "chip"), None), P(("node", "chip"), None, None)),
        check_vma=False,
    )
```
